32 devices in a mesh: fsdp: 4 (over y, x), seq: 8 (over z, core).
Axes of the slice: x: 2, y: 2, z: 4, core: 2. Of those that a mesh axis runs over, the one named last changes fastest.
Arguments:
- q_next: bfloat16 [4096, 4096], P(('fsdp', 'seq')), may hold values from -9 to 9
- k_next: bfloat16 [4096, 1024], P(('fsdp', 'seq')), may hold values from -4 to 4
- v_next: bfloat16 [4096, 1024], P(('fsdp', 'seq')), may hold values from -6 to 6
- seg_next: int32 [4, 1024], P('fsdp'), may hold values from 0 to 3, never falling along the last dimension, each value on 1 to 512 neighbouring positions
- q_prev: bfloat16 [4096, 4096], P(('fsdp', 'seq')), may hold values from -9 to 9
- k_prev: bfloat16 [4096, 1024], P(('fsdp', 'seq')), may hold values from -4 to 4
- v_prev: bfloat16 [4096, 1024], P(('fsdp', 'seq')), may hold values from -6 to 6
- seg_prev: int32 [4, 1024], P('fsdp'), may hold values from 0 to 3, never falling along the last dimension, each value on 1 to 512 neighbouring positions
- upstream: bfloat16 [4096, 4096], P(('fsdp', 'seq')), may hold values from -6 to 6
- flags: int32 [4, 1024], P('fsdp', 'seq'), may hold values from 0 to 1
Outputs:
- attn_next: bfloat16 [4096, 4096], P(('fsdp', 'seq'))
- grad_q: bfloat16 [4096, 4096], P(('fsdp', 'seq'))
- grad_k: bfloat16 [4096, 1024], P(('fsdp', 'seq'))
- grad_v: bfloat16 [4096, 1024], P(('fsdp', 'seq'))
The draws below stay inside these ranges and needn't reach their ends.
Inputs may be any that keep to these rules, and one draw needn't show every extreme that they name: `seg_next`: within each sequence the ids never fall and each id covers at most 512 consecutive positions; some id covers exactly 512. `seg_prev`: within each sequence the ids never fall and each id covers at most 512 consecutive positions; some id covers exactly 512.
All inputs are finite; a program needn't handle non-finite values.
Results may differ from the reference program's by a relative error of at most 0.0067.
Values may be sent and summed in bfloat16 or wider, within the bound.
No kernel may reach another device: no remote copies, remote signals or barrier semaphores. Data moves between devices by JAX's collectives and lax.ppermute only.
A program may use at most 128 MiB of HBM per device.

```python
import math
import jax
import jax.numpy as jnp
import numpy as np
from jax import lax

HEADS = 32
KV_HEADS = 8
HEAD_DIM = 128
TOK_DEV = 128
BATCH = 4
SEQ = 1024
TOKENS = 4096
SEG_MOST = 512
BLOCK = 512


def draw_pair(key, marker):
    key = jax.random.fold_in(key, marker)
    query_key, keys_key = jax.random.split(key, 2)
    queries = jnp.clip(jax.random.normal(query_key, (TOKENS, HEADS * HEAD_DIM), jnp.float32), -4.0, 4.0)
    keys_all = jnp.clip(jax.random.normal(keys_key, (TOKENS, KV_HEADS * HEAD_DIM), jnp.float32), -4.0, 4.0)
    return (queries.astype(jnp.bfloat16), keys_all.astype(jnp.bfloat16))


def draw_q_next(key, part):
    return draw_pair(key, 11)[0]


def draw_k_next(key, part):
    return draw_pair(key, 11)[1]


def draw_q_prev(key, part):
    return draw_pair(key, 23)[0]


def draw_k_prev(key, part):
    return draw_pair(key, 23)[1]


def draw_flags(key, part):
    key = jax.random.fold_in(key, 37)
    level_key, dice_key = jax.random.split(key)
    levels = jax.random.randint(level_key, (BATCH, SEQ // TOK_DEV), 4, 11)
    limits = jnp.left_shift(jnp.ones_like(levels), levels)
    limit_rows = jnp.repeat(limits, TOK_DEV, axis=1)
    dice = jax.random.randint(dice_key, (BATCH, SEQ), 0, 1024)
    return (dice < limit_rows).astype(jnp.int32)


def block_scale(rng, extent, shards, low, top_value):
    def one(axis_at, blocks):
        draws = jax.random.uniform(jax.random.fold_in(jax.random.fold_in(rng, 6), axis_at), (blocks,), jnp.float32, low / len(shards), top_value / len(shards))
        return jnp.repeat(jnp.exp(draws), extent[axis_at] // blocks).reshape((-1,) + (1,) * (len(extent) - axis_at - 1))

    factor_of = one(*shards[0])
    for cut in shards[1:]:
        factor_of = factor_of * one(*cut)
    return factor_of


def length_profile(count, total, most, lean):
    portions = [(1 << 20) // math.isqrt(grade ** lean) + 1 for grade in range(2, count + 1)]
    surplus, given = total - most - (count - 1), [1] * (count - 1)
    while surplus > 0:
        candidates = [i for i in range(count - 1) if given[i] < most]
        whole, left = sum([portions[i] for i in candidates]), surplus
        for i in candidates:
            addition = min(most - given[i], max(1, left * portions[i] // whole), surplus)
            given[i] = given[i] + addition
            surplus = surplus - addition
    return np.array([most] + given)


def ragged_sizes(key, count, total, most, lean):
    if count == 2:
        one = jax.random.randint(key, (), max(1, total - most), min(most, total - 1) + 1)
        return jnp.stack([one, total - one])
    tallies = jnp.asarray(length_profile(count, total, most, lean), jnp.int32)
    pairs = (count - 1) // 2
    giver, taker = tallies[1:1 + 2 * pairs:2], tallies[2:2 + 2 * pairs:2]
    slack = jnp.minimum(giver - 1, most - taker)
    shifted = jax.random.randint(jax.random.fold_in(key, 1), (pairs,), 0, 1 << 20) % (slack + 1)
    tallies = tallies.at[1:1 + 2 * pairs:2].set(giver - shifted).at[2:2 + 2 * pairs:2].set(taker + shifted)
    return tallies[jax.random.permutation(jax.random.fold_in(key, 2), count)]


def noise(rng, extent, deviation, limit, pieces=(), kind=jnp.bfloat16):
    gain = block_scale(rng, extent, pieces, -0.22, 0.18) if pieces else 1.0
    entries = jax.random.normal(rng, extent, jnp.float32) * deviation * gain
    return jnp.minimum(jnp.maximum(entries, -limit), limit).astype(kind)


def setup_inputs(seed: int = 0) -> dict:
    arg_keys = jax.random.split(jax.random.key(seed), 11)
    q_next = draw_q_next(jax.random.fold_in(arg_keys[10], 71), 0)
    k_next = draw_k_next(jax.random.fold_in(arg_keys[10], 71), 0)
    v_next = noise(arg_keys[2], (TOKENS, KV_HEADS * HEAD_DIM), 1.0, 6.0, ((0, 32),))
    seg_next = jax.vmap(lambda own: jnp.searchsorted(jnp.cumsum(ragged_sizes(own, 2 * SEQ // SEG_MOST, SEQ, SEG_MOST, 1)), jnp.arange(SEQ), side="right"))(jax.random.split(arg_keys[3], BATCH)).reshape((BATCH, SEQ)).astype(jnp.int32)
    q_prev = draw_q_prev(jax.random.fold_in(arg_keys[10], 71), 0)
    k_prev = draw_k_prev(jax.random.fold_in(arg_keys[10], 71), 0)
    v_prev = noise(arg_keys[6], (TOKENS, KV_HEADS * HEAD_DIM), 1.0, 6.0, ((0, 32),))
    seg_prev = jax.vmap(lambda own: jnp.searchsorted(jnp.cumsum(ragged_sizes(own, 2 * SEQ // SEG_MOST, SEQ, SEG_MOST, 1)), jnp.arange(SEQ), side="right"))(jax.random.split(arg_keys[7], BATCH)).reshape((BATCH, SEQ)).astype(jnp.int32)
    upstream = noise(arg_keys[8], (TOKENS, HEADS * HEAD_DIM), 1.0, 6.0, ((0, 32),))
    flags = draw_flags(jax.random.fold_in(arg_keys[10], 71), 0)
    return dict(q_next=q_next, k_next=k_next, v_next=v_next, seg_next=seg_next, q_prev=q_prev, k_prev=k_prev, v_prev=v_prev, seg_prev=seg_prev, upstream=upstream, flags=flags)


def narrow(values):
    return lax.optimization_barrier(values.astype(jnp.bfloat16)).astype(jnp.float32)


def masked_probs(q_block, k_window, q_pos, k_pos, q_seg, k_seg):
    scale_factor = HEAD_DIM ** -0.5
    scores = jnp.einsum('qhd,khd->hqk', q_block.astype(jnp.float32), k_window.astype(jnp.float32)) * scale_factor
    keep_mask = (k_seg[None, :] == q_seg[:, None]) & (k_pos[None, :] <= q_pos[:, None])
    scores = jnp.where(keep_mask[None], scores, -1e30)
    row_max = jnp.max(scores, axis=-1, keepdims=True)
    expo_vals = jnp.exp(scores - row_max)
    return expo_vals / jnp.sum(expo_vals, axis=-1, keepdims=True)


def block_window(seq_ids, block_start):
    padded = jnp.concatenate([jnp.full((SEG_MOST,), -1, jnp.int32), seq_ids.astype(jnp.int32)])
    q_seg = lax.dynamic_slice_in_dim(seq_ids.astype(jnp.int32), block_start, BLOCK)
    k_seg = lax.dynamic_slice_in_dim(padded, block_start, SEG_MOST + BLOCK)
    q_pos = block_start + jnp.arange(BLOCK, dtype=jnp.int32)
    k_pos = block_start - SEG_MOST + jnp.arange(SEG_MOST + BLOCK, dtype=jnp.int32)
    return q_pos, k_pos, q_seg, k_seg


def pad_front(array):
    return jnp.concatenate([jnp.zeros((SEG_MOST,) + array.shape[1:], array.dtype), array], axis=0)


def forward_heads(q_heads, k_heads, v_heads, seq_ids):
    k_padded = pad_front(k_heads)
    v_padded = pad_front(v_heads)

    def block_step(block_idx, output):
        block_start = (block_idx * BLOCK).astype(jnp.int32)
        q_pos, k_pos, q_seg, k_seg = block_window(seq_ids, block_start)
        q_block = lax.dynamic_slice_in_dim(q_heads, block_start, BLOCK, 0)
        k_window = lax.dynamic_slice_in_dim(k_padded, block_start, SEG_MOST + BLOCK, 0)
        v_window = lax.dynamic_slice_in_dim(v_padded, block_start, SEG_MOST + BLOCK, 0)
        soft_probs = masked_probs(q_block, k_window, q_pos, k_pos, q_seg, k_seg)
        result = jnp.einsum('hqk,khd->qhd', narrow(soft_probs), v_window.astype(jnp.float32)).astype(jnp.bfloat16)
        return lax.dynamic_update_slice_in_dim(output, result, block_start, 0)

    return lax.fori_loop(0, SEQ // BLOCK, block_step, jnp.zeros(q_heads.shape, jnp.bfloat16))


def backward_heads(q_heads, k_heads, v_heads, d_heads, seq_ids):
    k_padded = pad_front(k_heads)
    v_padded = pad_front(v_heads)
    scale_factor = HEAD_DIM ** -0.5

    def block_step(block_idx, carry):
        grad_qh, k_grads, v_grads = carry
        block_start = (block_idx * BLOCK).astype(jnp.int32)
        q_pos, k_pos, q_seg, k_seg = block_window(seq_ids, block_start)
        q_block = lax.dynamic_slice_in_dim(q_heads, block_start, BLOCK, 0).astype(jnp.float32)
        d_block = lax.dynamic_slice_in_dim(d_heads, block_start, BLOCK, 0).astype(jnp.float32)
        k_window = lax.dynamic_slice_in_dim(k_padded, block_start, SEG_MOST + BLOCK, 0).astype(jnp.float32)
        v_window = lax.dynamic_slice_in_dim(v_padded, block_start, SEG_MOST + BLOCK, 0).astype(jnp.float32)
        soft_probs = masked_probs(q_block, k_window, q_pos, k_pos, q_seg, k_seg)
        d_probs = jnp.einsum('qhd,khd->hqk', d_block, v_window)
        row_delta = jnp.sum(soft_probs * d_probs, axis=-1, keepdims=True)
        d_scores = narrow(soft_probs * (d_probs - row_delta) * scale_factor)
        q_grad = jnp.einsum('hqk,khd->qhd', d_scores, k_window).astype(jnp.bfloat16)
        k_term = jnp.einsum('hqk,qhd->khd', d_scores, q_block)
        v_term = jnp.einsum('hqk,qhd->khd', narrow(soft_probs), d_block)
        grad_qh = lax.dynamic_update_slice_in_dim(grad_qh, q_grad, block_start, 0)
        k_old = lax.dynamic_slice_in_dim(k_grads, block_start, SEG_MOST + BLOCK, 0)
        v_old = lax.dynamic_slice_in_dim(v_grads, block_start, SEG_MOST + BLOCK, 0)
        k_grads = lax.dynamic_update_slice_in_dim(k_grads, k_old + k_term, block_start, 0)
        v_grads = lax.dynamic_update_slice_in_dim(v_grads, v_old + v_term, block_start, 0)
        return grad_qh, k_grads, v_grads

    buffer_shape = (SEG_MOST + SEQ,) + q_heads.shape[1:]
    start_carry = (jnp.zeros(q_heads.shape, jnp.bfloat16), jnp.zeros(buffer_shape, jnp.float32), jnp.zeros(buffer_shape, jnp.float32))
    grad_qh, k_grads, v_grads = lax.fori_loop(0, SEQ // BLOCK, block_step, start_carry)
    return grad_qh, k_grads[SEG_MOST:], v_grads[SEG_MOST:]


def reference(q_next, k_next, v_next, seg_next, q_prev, k_prev, v_prev, seg_prev, upstream, flags):
    group_size = HEADS // KV_HEADS

    def query_heads(array):
        return array.reshape(BATCH, SEQ, HEADS, HEAD_DIM)

    def shared_heads(array):
        return jnp.repeat(array.reshape(BATCH, SEQ, KV_HEADS, HEAD_DIM), group_size, axis=2)

    def group_sum(array):
        summed = jnp.sum(array.reshape(TOKENS, KV_HEADS, group_size, HEAD_DIM).astype(jnp.float32), axis=2)
        return summed.astype(jnp.bfloat16).reshape(TOKENS, KV_HEADS * HEAD_DIM)

    attn = lax.map(lambda members: forward_heads(*members), (query_heads(q_next), shared_heads(k_next), shared_heads(v_next), seg_next))
    attn_next = attn.reshape(TOKENS, HEADS * HEAD_DIM)
    flag_total = jnp.sum(flags.astype(jnp.float32))
    weight = flags.reshape(TOKENS, 1).astype(jnp.float32) * (TOKENS / jnp.maximum(flag_total, 1.0))
    cotangent = (upstream.astype(jnp.float32) * weight).astype(jnp.bfloat16)
    grads = lax.map(lambda members: backward_heads(*members), (query_heads(q_prev), shared_heads(k_prev), shared_heads(v_prev), query_heads(cotangent), seg_prev))
    grad_q = grads[0].reshape(TOKENS, HEADS * HEAD_DIM)
    grad_k = group_sum(grads[1])
    grad_v = group_sum(grads[2])
    return attn_next, grad_q, grad_k, grad_v
```

```python
import functools
import math

import jax
import jax.numpy as jnp
from jax import lax
from jax.experimental import pallas as pl
from jax.experimental.pallas import tpu as pltpu
from jax.sharding import PartitionSpec as P

HEAD_DIM = 128
SEG_MOST = 512
SLOTS = 5
NEG = -1e30


def shifted(block, step):
    size = lax.axis_size("seq")
    return lax.ppermute(
        block, "seq", [(i, i + step) for i in range(size) if 0 <= i + step < size]
    )


def swapped(block, from_even=True, from_odd=True):
    size = lax.axis_size("seq")
    route = [(i, i ^ 1) for i in range(size) if (from_odd if i % 2 else from_even)]
    return lax.ppermute(block, "seq", route)


def total_over(value, axis):
    size, step = lax.axis_size(axis), 1
    while step < size:
        route = [(i, i ^ step) for i in range(size)]
        value = value + lax.ppermute(value, axis, route)
        step *= 2
    return value


def mask_bias(seq_ids, rows_here):
    index = lax.axis_index("seq")
    odd = index % 2
    first = index * rows_here
    q_seg = lax.dynamic_slice_in_dim(seq_ids, first, rows_here)
    start = jnp.sum((seq_ids[:, None] < q_seg[None, :]).astype(jnp.int32), axis=0)
    q_pos = first + jnp.arange(rows_here, dtype=jnp.int32)
    back = jnp.stack(
        [
            jnp.int32(4),
            3 - 2 * odd,
            jnp.int32(2),
            1 + 2 * odd,
            jnp.int32(0),
        ]
    )
    k_pos = (first - back * rows_here)[:, None] + jnp.arange(rows_here, dtype=jnp.int32)
    k_pos = k_pos[:, :, None]
    keep = (k_pos >= start) & (k_pos <= q_pos)
    return jnp.where(keep, 0.0, NEG).astype(jnp.float32).reshape(SLOTS * rows_here, rows_here)


def gather_window(odd, refs, columns):
    far, far_x, mid, near_y, own, near_x = refs
    x_slot = jnp.where(odd == 1, near_x[:, columns], far_x[:, columns])
    return jnp.concatenate(
        [far[:, columns], x_slot, mid[:, columns], near_y[:, columns], own[:, columns]], axis=0
    )


def column(start):
    return pl.ds(pl.multiple_of(start, HEAD_DIM), HEAD_DIM)


def stacked_heads(ref, kv_head, group):
    return jnp.concatenate(
        [ref[:, column((kv_head * group + t) * HEAD_DIM)] for t in range(group)], axis=0
    )


def exp_scores(keys, queries, bias, group, factor):
    scores = lax.dot_general(
        keys, queries, (((1,), (1,)), ((), ())), preferred_element_type=jnp.float32
    )
    scores = scores * factor + jnp.concatenate([bias] * group, axis=1)
    return jnp.exp2(scores - jnp.max(scores, axis=0, keepdims=True))


def forward_kernel(group, kv_heads, factor, odd_ref, bias_ref, q_ref, *refs):
    window, out_ref = refs[:6], refs[6]
    odd = odd_ref[0]

    def one(g, carry):
        keys = gather_window(odd, window, column(g * HEAD_DIM))
        values = gather_window(odd, window, column((kv_heads + g) * HEAD_DIM))
        queries = stacked_heads(q_ref, g, group)
        expo = exp_scores(keys, queries, bias_ref[...], group, factor)
        total = jnp.sum(expo, axis=0, keepdims=True)
        out = lax.dot_general(
            values,
            expo.astype(jnp.bfloat16),
            (((0,), (0,)), ((), ())),
            preferred_element_type=jnp.float32,
        )
        out = out * (1.0 / total)
        rows = q_ref.shape[0]
        for t in range(group):
            out_ref[:, column((g * group + t) * HEAD_DIM)] = (
                out[:, t * rows : (t + 1) * rows].T.astype(out_ref.dtype)
            )
        return carry

    lax.fori_loop(0, kv_heads, one, 0)


def backward_kernel(group, kv_heads, factor, scale, odd_ref, bias_ref, q_ref, d_ref, *refs):
    window, dq_ref, outs = refs[:6], refs[6], refs[7:]
    odd = odd_ref[0]
    rows = q_ref.shape[0]

    def one(g, carry):
        k_col, v_col = column(g * HEAD_DIM), column((kv_heads + g) * HEAD_DIM)
        keys = gather_window(odd, window, k_col)
        values = gather_window(odd, window, v_col)
        queries = stacked_heads(q_ref, g, group)
        cots = stacked_heads(d_ref, g, group)
        expo = exp_scores(keys, queries, bias_ref[...], group, factor)
        d_probs = lax.dot_general(
            values, cots, (((1,), (1,)), ((), ())), preferred_element_type=jnp.float32
        )
        probs = expo * (1.0 / jnp.sum(expo, axis=0, keepdims=True))
        delta = jnp.sum(probs * d_probs, axis=0, keepdims=True)
        d_scores = (probs * (d_probs - delta) * scale).astype(jnp.bfloat16)
        dv = jnp.dot(probs.astype(jnp.bfloat16), cots, preferred_element_type=jnp.float32)
        dk = jnp.dot(d_scores, queries, preferred_element_type=jnp.float32)
        dq = lax.dot_general(
            keys, d_scores, (((0,), (0,)), ((), ())), preferred_element_type=jnp.float32
        )
        for t in range(group):
            dq_ref[:, column((g * group + t) * HEAD_DIM)] = (
                dq[:, t * rows : (t + 1) * rows].T.astype(dq_ref.dtype)
            )
        for s, ref in enumerate(outs):
            ref[:, k_col] = dk[s * rows : (s + 1) * rows].astype(ref.dtype)
            ref[:, v_col] = dv[s * rows : (s + 1) * rows].astype(ref.dtype)
        return carry

    lax.fori_loop(0, kv_heads, one, 0)


def call(kernel, outs, smem, *args):
    vmem = pl.BlockSpec(memory_space=pltpu.VMEM)
    return pl.pallas_call(
        kernel,
        out_shape=outs,
        in_specs=[pl.BlockSpec(memory_space=pltpu.SMEM)] + [vmem] * len(args),
        out_specs=jax.tree.map(lambda _: vmem, outs),
        compiler_params=pltpu.CompilerParams(vmem_limit_bytes=48 << 20),
    )(smem, *args)


def fetch_window(kv):
    mid = shifted(kv, 2)
    near_x = swapped(kv, from_odd=False)
    far = shifted(mid, 2)
    near_y = swapped(mid)
    far_x = swapped(far, from_even=False)
    return far, far_x, mid, near_y, kv, near_x


def body(q_next, k_next, v_next, seg_next, q_prev, k_prev, v_prev, seg_prev, upstream, flags):
    rows_here = q_next.shape[0]
    heads_all = q_next.shape[1] // HEAD_DIM
    kv_heads = k_next.shape[1] // HEAD_DIM
    group = heads_all // kv_heads
    seq_size = lax.axis_size("seq")
    token_total = rows_here * lax.axis_size("fsdp") * seq_size
    assert seq_size % 2 == 0 and SEG_MOST <= 4 * rows_here
    scale = HEAD_DIM ** (-0.5)
    factor = scale * math.log2(math.e)
    odd = lax.axis_index("seq") % 2
    odd_s = odd.reshape(1).astype(jnp.int32)

    kv_prev = jnp.concatenate([k_prev, v_prev], axis=1)
    kv_next = jnp.concatenate([k_next, v_next], axis=1)
    window_prev = fetch_window(kv_prev)
    window_next = fetch_window(kv_next)

    count = jnp.sum(flags.astype(jnp.float32)).reshape(1, 1) * jnp.ones((1, 128), jnp.float32)
    flag_total = total_over(total_over(count, "fsdp"), "seq")[0, 0]
    weight = flags.reshape(rows_here, 1).astype(jnp.float32) * (
        token_total / jnp.maximum(flag_total, 1.0)
    )
    cotangent = (upstream.astype(jnp.float32) * weight).astype(jnp.bfloat16)
    bias_prev = mask_bias(seg_prev[0], rows_here)
    bias_next = mask_bias(seg_next[0], rows_here)

    kv_shape = kv_prev.shape
    f32_kv = jax.ShapeDtypeStruct(kv_shape, jnp.float32)
    b16_kv = jax.ShapeDtypeStruct(kv_shape, jnp.bfloat16)
    q_shape = jax.ShapeDtypeStruct(q_prev.shape, jnp.bfloat16)
    grad_q, far, x_part, mid, y_part, own = call(
        functools.partial(backward_kernel, group, kv_heads, factor, scale),
        (q_shape, f32_kv, b16_kv, f32_kv, b16_kv, f32_kv),
        odd_s,
        bias_prev,
        q_prev,
        cotangent,
        *window_prev,
    )
    x_back = swapped(x_part).astype(jnp.float32)
    y_back = swapped(y_part).astype(jnp.float32)
    is_odd = odd == 1
    far = (far + jnp.where(is_odd, x_back, 0.0)).astype(jnp.bfloat16)
    mid = (mid + y_back + shifted(far, -2).astype(jnp.float32)).astype(jnp.bfloat16)
    own = own + jnp.where(is_odd, 0.0, x_back) + shifted(mid, -2).astype(jnp.float32)
    own = own.astype(jnp.bfloat16)
    split = k_prev.shape[1]

    attn_next = call(
        functools.partial(forward_kernel, group, kv_heads, factor),
        q_shape,
        odd_s,
        bias_next,
        q_next,
        *window_next,
    )
    return (attn_next, grad_q, own[:, :split], own[:, split:])


def solution(mesh):
    tokens = P(("fsdp", "seq"), None)
    ids = P("fsdp", None)
    return jax.shard_map(
        body,
        mesh=mesh,
        in_specs=(tokens, tokens, tokens, ids) * 2 + (tokens, P("fsdp", "seq")),
        out_specs=(tokens,) * 4,
        check_vma=False,
    )
```

```python
import functools
import math

import jax
import jax.numpy as jnp
from jax import lax
from jax.experimental import pallas as pl
from jax.experimental.pallas import tpu as pltpu
from jax.sharding import PartitionSpec as P


HEAD_DIM = 128
SEG_MOST = 512
SLOTS = 5
NEG = -1e30
VMEM_LIMIT = 12 << 20


def shifted(block, step, second=False):
    size = lax.axis_size("seq")
    route = [(i, i + step) for i in range(size) if 0 <= i + step < size]
    if second:
        route = [(i, j) for i, j in route if 0 <= i - abs(step)]
    return lax.ppermute(block, "seq", route)


def returned(block):
    route = [(i, i - 2) for i in range(4, lax.axis_size("seq"))]
    return lax.ppermute(block, "seq", route)


def swapped(block):
    route = [(i, i ^ 1) for i in range(lax.axis_size("seq"))]
    return lax.ppermute(block, "seq", route)


def column(start):
    return pl.ds(pl.multiple_of(start, HEAD_DIM), HEAD_DIM)


def gather_window(odd, refs, columns):
    far, far_x, mid, near_y, own, near_x = refs
    x_slot = jnp.where(odd == 1, near_x[:, columns], far_x[:, columns])
    return jnp.concatenate(
        [far[:, columns], x_slot, mid[:, columns], near_y[:, columns], own[:, columns]], axis=0
    )


def stacked_heads(ref, kv_head, group):
    return jnp.concatenate(
        [ref[:, column((kv_head * group + t) * HEAD_DIM)] for t in range(group)], axis=0
    )


def contract(left, right, left_dim, right_dim):
    return lax.dot_general(
        left,
        right,
        (((left_dim,), (right_dim,)), ((), ())),
        preferred_element_type=jnp.float32,
    )


def staged(count, *stages):
    for step in range(count + len(stages) - 1):
        for depth in reversed(range(len(stages))):
            if 0 <= step - depth < count:
                stages[depth](step - depth)


def soften(scores_ref, bias_ref, expo_ref, group, factor, normalised):
    rows = bias_ref.shape[1]
    inverses = []
    for t in range(group):
        cols = slice(t * rows, (t + 1) * rows)
        scores = scores_ref[:, cols] * factor + bias_ref[...]
        expo = jnp.exp2(scores - jnp.max(scores, axis=0, keepdims=True))
        inverse = 1.0 / jnp.sum(expo, axis=0, keepdims=True)
        expo_ref[:, cols] = (expo * inverse if normalised else expo).astype(expo_ref.dtype)
        inverses.append(inverse)
    return inverses


def upright(row):
    return jnp.broadcast_to(row, (HEAD_DIM, HEAD_DIM)).T


def prep_kernel(index_ref, *refs):
    prev_hbm, next_hbm, flags_hbm, up_hbm, qp_hbm, kp_hbm, vp_hbm, qn_hbm, kn_hbm, vn_hbm = refs[:10]
    bias_prev_ref, bias_next_ref, count_ref, cots_ref, qp_ref, kp_ref, vp_ref = refs[10:17]
    qn_ref, kv_ref, prev_ref, next_ref, flags_ref, up_ref, sems = refs[17:]
    width = kn_hbm.shape[1]
    moves = (
        (prev_hbm, prev_ref),
        (next_hbm, next_ref),
        (flags_hbm, flags_ref),
        (up_hbm, up_ref),
        (qp_hbm, qp_ref),
        (kp_hbm, kp_ref),
        (vp_hbm, vp_ref),
        (kn_hbm, kv_ref.at[:, :width]),
        (vn_hbm, kv_ref.at[:, width:]),
        (qn_hbm, qn_ref),
    )
    copies = [pltpu.make_async_copy(a, b, sems.at[i]) for i, (a, b) in enumerate(moves)]
    for copy in copies:
        copy.start()
    index = index_ref[0]
    odd = index % 2
    rows = flags_ref.shape[1]
    far = jnp.iinfo(jnp.int32).max // 2
    key_at = lax.broadcasted_iota(jnp.int32, (rows, rows), 0)
    query_at = lax.broadcasted_iota(jnp.int32, (rows, rows), 1)
    for copy in copies[:3]:
        copy.wait()
    for seg_ref, bias_ref in ((prev_ref, bias_prev_ref), (next_ref, bias_next_ref)):
        queries = seg_ref[:, column(index * rows)].astype(jnp.float32)
        for slot, back in enumerate((4, 3 - 2 * odd, 2, 1 + 2 * odd, 0)):
            block = index - back
            first = jnp.where(block >= 0, -back * rows, far)
            keys = upright(seg_ref[:, column(jnp.maximum(block, 0) * rows)].astype(jnp.float32))
            keep = (keys == queries) & (key_at + first <= query_at)
            bias_ref[slot * rows : (slot + 1) * rows, :] = jnp.where(keep, 0.0, NEG)
    flagged = flags_ref[...].astype(jnp.float32)
    count = jnp.sum(flagged, axis=1, keepdims=True)
    count_ref[...] = jnp.broadcast_to(count, count_ref.shape)
    keep = upright(flagged).astype(jnp.bfloat16)
    copies[3].wait()
    for h in range(up_ref.shape[1] // HEAD_DIM):
        cols = slice(h * HEAD_DIM, (h + 1) * HEAD_DIM)
        cots_ref[:, cols] = up_ref[:, cols] * keep
    for copy in copies[4:]:
        copy.wait()


def add_kernel(left_ref, right_ref, out_ref):
    out_ref[...] = left_ref[...] + right_ref[...]


def gain_kernel(tokens, left_ref, right_ref, out_ref):
    out_ref[...] = tokens / jnp.maximum(left_ref[...] + right_ref[...], 1.0)


def forward_kernel(plan, odd_ref, bias_ref, q_ref, *refs):
    group, heads, factor, _ = plan
    window, (out_ref, held, sems, scores_buf, expo_buf) = refs[:6], refs[6:]
    odd = odd_ref[0]
    rows = q_ref.shape[0]
    wide = group * HEAD_DIM
    inverses = {}

    def sent(g):
        cols = slice(g * wide, (g + 1) * wide)
        return pltpu.make_async_copy(held.at[:, cols], out_ref.at[:, cols], sems.at[g])

    def scores(g):
        keys = gather_window(odd, window, column(g * HEAD_DIM))
        scores_buf[g % 2] = contract(keys, stacked_heads(q_ref, g, group), 1, 1)

    def softmax(g):
        views = scores_buf.at[g % 2], bias_ref, expo_buf.at[g % 2]
        inverses[g] = soften(*views, group, factor, False)

    def output(g):
        values = gather_window(odd, window, column((heads + g) * HEAD_DIM))
        out = contract(values, expo_buf[g % 2], 0, 0)
        for t in range(group):
            piece = out[:, t * rows : (t + 1) * rows] * inverses[g][t]
            held[:, column((g * group + t) * HEAD_DIM)] = piece.T.astype(held.dtype)
        sent(g).start()

    staged(heads, scores, softmax, output)
    for g in range(heads):
        sent(g).wait()


def last_kernel(odd_ref, gain_ref, *refs):
    sums, outs = refs[:6], refs[6:]
    for i, out_ref in enumerate(outs):
        own, other, back = sums[3 * i : 3 * i + 3]
        share = jnp.where(odd_ref[0] == 0, other[...].astype(jnp.float32), 0.0)
        total = own[...] + share + back[...].astype(jnp.float32)
        gain = jnp.concatenate([gain_ref[...]] * (total.shape[1] // HEAD_DIM), axis=1)
        out_ref[...] = (total * gain).astype(out_ref.dtype)


def probs_kernel(plan, odd_ref, bias_ref, q_ref, d_ref, *refs):
    group, heads, factor, _ = plan
    window, (p_ref, outs, scores_buf) = refs[:6], (refs[6], refs[7:-1], refs[-1])
    odd = odd_ref[0]
    rows = q_ref.shape[0]

    def scores(g):
        keys = gather_window(odd, window, column(g * HEAD_DIM))
        scores_buf[g % 2] = contract(keys, stacked_heads(q_ref, g, group), 1, 1)

    def softmax(g):
        soften(scores_buf.at[g % 2], bias_ref, p_ref.at[g], group, factor, True)

    def gradients(g):
        dv = contract(p_ref[g], stacked_heads(d_ref, g, group), 1, 0)
        for s, ref in enumerate(outs):
            ref[:, column(g * HEAD_DIM)] = dv[s * rows : (s + 1) * rows].astype(ref.dtype)

    staged(heads, scores, softmax, gradients)


def scores_kernel(plan, odd_ref, q_ref, d_ref, p_ref, *refs):
    group, heads, _, scale = plan
    window, (s_ref, far_ref, x_ref, probs_buf) = refs[:6], refs[6:]
    odd = odd_ref[0]
    rows = q_ref.shape[0]

    def products(g):
        values = gather_window(odd, window, column(g * HEAD_DIM))
        probs_buf[g % 2] = contract(values, stacked_heads(d_ref, g, group), 1, 1)

    def scores(g):
        for t in range(group):
            cols = slice(t * rows, (t + 1) * rows)
            d_probs = probs_buf[g % 2, :, cols]
            probs = p_ref[g, :, cols].astype(jnp.float32)
            delta = jnp.sum(probs * d_probs, axis=0, keepdims=True)
            s_ref[g, :, cols] = (probs * (d_probs - delta)).astype(s_ref.dtype)

    def gradients(g):
        cols = column(g * HEAD_DIM)
        dk = contract(s_ref[g, : 2 * rows, :], stacked_heads(q_ref, g, group), 1, 0) * scale
        far_ref[:, cols] = dk[:rows].astype(far_ref.dtype)
        x_ref[:, cols] = dk[rows:].astype(x_ref.dtype)

    staged(heads, products, scores, gradients)


def keys_kernel(plan, q_ref, s_ref, mid_ref, y_ref, own_ref):
    group, heads, _, scale = plan
    rows = q_ref.shape[0]

    def one(g, carry):
        cols = column(g * HEAD_DIM)
        queries = stacked_heads(q_ref, g, group)
        dk = contract(s_ref[g, 2 * rows :, :], queries, 1, 0) * scale
        for s, ref in enumerate((mid_ref, y_ref, own_ref)):
            ref[:, cols] = dk[s * rows : (s + 1) * rows].astype(ref.dtype)
        return carry

    lax.fori_loop(0, heads, one, 0, unroll=4)


def queries_kernel(plan, odd_ref, gain_ref, s_ref, *refs):
    group, heads, _, scale = plan
    window, (dq_ref, held, sems) = refs[:6], refs[6:]
    odd = odd_ref[0]
    rows = gain_ref.shape[1]
    wide = group * HEAD_DIM
    gain = gain_ref[...] * scale

    def sent(g):
        cols = pl.ds(pl.multiple_of(g * wide, wide), wide)
        return pltpu.make_async_copy(held.at[:, cols], dq_ref.at[:, cols], sems.at[g])

    def one(g, carry):
        keys = gather_window(odd, window, column(g * HEAD_DIM))
        dq = contract(keys, s_ref[g], 0, 0)
        for t in range(group):
            piece = dq[:, t * rows : (t + 1) * rows].T * gain
            held[:, column((g * group + t) * HEAD_DIM)] = piece.astype(held.dtype)
        sent(g).start()
        return carry

    lax.fori_loop(0, heads, one, 0, unroll=4)
    for g in range(heads):
        sent(g).wait()


def far_kernel(odd_ref, far_ref, x_ref, out_ref):
    share = jnp.where(odd_ref[0] == 1, x_ref[...].astype(jnp.float32), 0.0)
    out_ref[...] = (far_ref[...] + share).astype(out_ref.dtype)


def mid_kernel(mid_ref, y_ref, back_ref, out_ref):
    total = mid_ref[...] + y_ref[...].astype(jnp.float32) + back_ref[...].astype(jnp.float32)
    out_ref[...] = total.astype(out_ref.dtype)


def call(kernel, outs, smem, args, in_hbm=(), out_hbm=(), scratch=()):
    vmem = pl.BlockSpec(memory_space=pltpu.VMEM)
    scalar = pl.BlockSpec(memory_space=pltpu.SMEM)
    hbm = pl.BlockSpec(memory_space=pltpu.HBM)
    args = [
        pltpu.with_memory_space_constraint(x, pltpu.HBM) if i in in_hbm else x
        for i, x in enumerate(args)
    ]
    return pl.pallas_call(
        kernel,
        out_shape=tuple(outs) if len(outs) > 1 else outs[0],
        in_specs=[scalar] * len(smem)
        + [hbm if i in in_hbm else vmem for i in range(len(args))],
        out_specs=tuple(hbm if i in out_hbm else vmem for i in range(len(outs)))
        if len(outs) > 1
        else (hbm if out_hbm else vmem),
        scratch_shapes=list(scratch),
        compiler_params=pltpu.CompilerParams(vmem_limit_bytes=VMEM_LIMIT),
    )(*smem, *args)


def fetch_window(block, mid):
    near_x = swapped(block)
    far = shifted(mid, 2, second=True)
    near_y = swapped(mid)
    far_x = swapped(far)
    return far, far_x, mid, near_y, block, near_x


def body(q_next, k_next, v_next, seg_next, q_prev, k_prev, v_prev, seg_prev, upstream, flags):
    rows = q_next.shape[0]
    heads_all = q_next.shape[1] // HEAD_DIM
    heads = k_next.shape[1] // HEAD_DIM
    group = heads_all // heads
    seq_size, fsdp_size = lax.axis_size("seq"), lax.axis_size("fsdp")
    tokens = rows * fsdp_size * seq_size
    assert seq_size % 2 == 0 and SEG_MOST <= 4 * rows and rows == HEAD_DIM
    scale = HEAD_DIM ** (-0.5)
    plan = (group, heads, scale * math.log2(math.e), scale)
    index = lax.axis_index("seq").astype(jnp.int32).reshape(1)
    odd = index % 2
    b16, f32 = jnp.bfloat16, jnp.float32

    def sds(shape, dtype):
        return jax.ShapeDtypeStruct(shape, dtype)

    k_shape, v_shape = k_prev.shape, v_prev.shape
    wide = group * rows
    scores_scratch = pltpu.VMEM((2, SLOTS * rows, wide), f32)
    out_scratch = (pltpu.VMEM(q_prev.shape, b16), pltpu.SemaphoreType.DMA((heads,)))

    keys_out, values_out = (shifted(x, 2) for x in (k_prev, v_prev))
    bias_shape = sds((SLOTS * rows, rows), f32)
    line = sds((1, HEAD_DIM), f32)
    staged = (seg_prev, seg_next, flags, upstream, q_prev, k_prev, v_prev, q_next, k_next, v_next)
    bias_prev, bias_next, count, cots, q_prev, k_here, v_here, q_next, kv_next = call(
        prep_kernel,
        (
            bias_shape,
            bias_shape,
            line,
            sds(upstream.shape, b16),
            sds(q_prev.shape, b16),
            sds(k_shape, b16),
            sds(v_shape, b16),
            sds(q_next.shape, b16),
            sds((rows, 2 * k_next.shape[1]), b16),
        ),
        (index,),
        staged,
        in_hbm=range(len(staged)),
        scratch=tuple(pltpu.VMEM(x.shape, x.dtype) for x in staged[:4])
        + (pltpu.SemaphoreType.DMA((len(staged),)),),
    )
    keys = fetch_window(k_here, keys_out)
    values = fetch_window(v_here, values_out)
    window_next = fetch_window(kv_next, shifted(kv_next, 2))
    steps = [("fsdp", 1 << i) for i in range((fsdp_size - 1).bit_length())]
    steps += [("seq", 1 << i) for i in range(1, (seq_size - 1).bit_length())] + [("seq", 1)]
    for at, (axis, step) in enumerate(steps):
        route = [(i, i ^ step) for i in range(lax.axis_size(axis))]
        other = lax.ppermute(count, axis, route)
        last = at == len(steps) - 1
        kernel = functools.partial(gain_kernel, tokens) if last else add_kernel
        count = call(kernel, (line,), (), (count, other))
    gain = count

    probs, far_v, x_v, mid_v, y_v, own_v = call(
        functools.partial(probs_kernel, plan),
        (
            sds((heads, SLOTS * rows, wide), b16),
            sds(v_shape, f32),
            sds(v_shape, b16),
            sds(v_shape, f32),
            sds(v_shape, b16),
            sds(v_shape, f32),
        ),
        (odd,),
        (bias_prev, q_prev, cots, *keys),
        scratch=(scores_scratch,),
    )
    x_v, y_v = swapped(x_v), swapped(y_v)
    far_v = call(far_kernel, (sds(v_shape, b16),), (odd,), (far_v, x_v))
    far_v = returned(far_v)

    d_scores, far_k, x_k = call(
        functools.partial(scores_kernel, plan),
        (sds(probs.shape, b16), sds(k_shape, f32), sds(k_shape, b16)),
        (odd,),
        (q_prev, cots, probs, *values),
        scratch=(scores_scratch,),
    )
    x_k = swapped(x_k)
    far_k = call(far_kernel, (sds(k_shape, b16),), (odd,), (far_k, x_k))
    far_k = returned(far_k)

    mid_v = call(mid_kernel, (sds(v_shape, b16),), (), (mid_v, y_v, far_v))
    mid_v = shifted(mid_v, -2)
    mid_k, y_k, own_k = call(
        functools.partial(keys_kernel, plan),
        (sds(k_shape, f32), sds(k_shape, b16), sds(k_shape, f32)),
        (),
        (q_prev, d_scores),
    )
    y_k = swapped(y_k)
    grad_q = call(
        functools.partial(queries_kernel, plan),
        (sds(q_prev.shape, b16),),
        (odd,),
        (gain, d_scores, *keys),
        out_hbm=(0,),
        scratch=out_scratch,
    )
    mid_k = call(mid_kernel, (sds(k_shape, b16),), (), (mid_k, y_k, far_k))
    mid_k = shifted(mid_k, -2)

    attn_next = call(
        functools.partial(forward_kernel, plan),
        (sds(q_next.shape, b16),),
        (odd,),
        (bias_next, q_next, *window_next),
        out_hbm=(0,),
        scratch=out_scratch + (scores_scratch, pltpu.VMEM((2, SLOTS * rows, wide), b16)),
    )
    grad_k, grad_v = call(
        last_kernel,
        (sds(k_shape, b16), sds(v_shape, b16)),
        (odd,),
        (gain, own_k, x_k, mid_k, own_v, x_v, mid_v),
    )
    return (attn_next, grad_q, grad_k, grad_v)


def solution(mesh):
    tokens = P(("fsdp", "seq"), None)
    ids = P("fsdp", None)
    return jax.shard_map(
        body,
        mesh=mesh,
        in_specs=(tokens, tokens, tokens, ids) * 2 + (tokens, P("fsdp", "seq")),
        out_specs=(tokens,) * 4,
        check_vma=False,
    )
```

```python
import functools
import math

import jax
import jax.numpy as jnp
from jax import lax
from jax.experimental import pallas as pl
from jax.experimental.pallas import tpu as pltpu
from jax.sharding import PartitionSpec as P


HEAD_DIM = 128
SEG_MOST = 512
SLOTS = 5
NEG = -1e30
VMEM_LIMIT = 12 << 20


def shifted(block, step, second=False):
    size = lax.axis_size("seq")
    route = [(i, i + step) for i in range(size) if 0 <= i + step < size]
    if second:
        route = [(i, j) for i, j in route if 0 <= i - abs(step)]
    return lax.ppermute(block, "seq", route)


def returned(block):
    route = [(i, i - 2) for i in range(4, lax.axis_size("seq"))]
    return lax.ppermute(block, "seq", route)


def swapped(block):
    route = [(i, i ^ 1) for i in range(lax.axis_size("seq"))]
    return lax.ppermute(block, "seq", route)


def column(start):
    return pl.ds(pl.multiple_of(start, HEAD_DIM), HEAD_DIM)


def gather_window(odd, refs, columns):
    far, far_x, mid, near_y, own, near_x = refs
    x_slot = jnp.where(odd == 1, near_x[:, columns], far_x[:, columns])
    return jnp.concatenate(
        [far[:, columns], x_slot, mid[:, columns], near_y[:, columns], own[:, columns]], axis=0
    )


def stacked_heads(ref, kv_head, group):
    return jnp.concatenate(
        [ref[:, column((kv_head * group + t) * HEAD_DIM)] for t in range(group)], axis=0
    )


def contract(left, right, left_dim, right_dim):
    return lax.dot_general(
        left,
        right,
        (((left_dim,), (right_dim,)), ((), ())),
        preferred_element_type=jnp.float32,
    )


def staged(count, *stages):
    for step in range(count + len(stages) - 1):
        for depth in reversed(range(len(stages))):
            if 0 <= step - depth < count:
                stages[depth](step - depth)


def soften(scores_ref, bias_ref, expo_ref, group, factor):
    rows = bias_ref.shape[1]
    for t in range(group):
        cols = slice(t * rows, (t + 1) * rows)
        scores = scores_ref[:, cols] * factor + bias_ref[...]
        expo = jnp.exp2(scores - jnp.max(scores, axis=0, keepdims=True))
        inverse = 1.0 / jnp.sum(expo, axis=0, keepdims=True)
        expo_ref[:, cols] = (expo * inverse).astype(expo_ref.dtype)


def upright(row):
    return jnp.broadcast_to(row, (HEAD_DIM, HEAD_DIM)).T


def prep_kernel(index_ref, *refs):
    prev_hbm, next_hbm, flags_hbm, up_hbm, qp_hbm, kp_hbm, vp_hbm, qn_hbm, kn_hbm, vn_hbm = refs[:10]
    bias_prev_ref, bias_next_ref, count_ref, cots_ref, qp_ref, kp_ref, vp_ref = refs[10:17]
    qn_ref, kv_ref, prev_ref, next_ref, flags_ref, up_ref, sems = refs[17:]
    width = kn_hbm.shape[1]
    moves = (
        (prev_hbm, prev_ref),
        (next_hbm, next_ref),
        (flags_hbm, flags_ref),
        (up_hbm, up_ref),
        (qp_hbm, qp_ref),
        (kp_hbm, kp_ref),
        (vp_hbm, vp_ref),
        (kn_hbm, kv_ref.at[:, :width]),
        (vn_hbm, kv_ref.at[:, width:]),
        (qn_hbm, qn_ref),
    )
    copies = [pltpu.make_async_copy(a, b, sems.at[i]) for i, (a, b) in enumerate(moves)]
    for copy in copies:
        copy.start()
    index = index_ref[0]
    odd = index % 2
    rows = flags_ref.shape[1]
    far = jnp.iinfo(jnp.int32).max // 2
    key_at = lax.broadcasted_iota(jnp.int32, (rows, rows), 0)
    query_at = lax.broadcasted_iota(jnp.int32, (rows, rows), 1)
    for copy in copies[:3]:
        copy.wait()
    for seg_ref, bias_ref in ((prev_ref, bias_prev_ref), (next_ref, bias_next_ref)):
        queries = seg_ref[:, column(index * rows)].astype(jnp.float32)
        for slot, back in enumerate((4, 3 - 2 * odd, 2, 1 + 2 * odd, 0)):
            block = index - back
            first = jnp.where(block >= 0, -back * rows, far)
            keys = upright(seg_ref[:, column(jnp.maximum(block, 0) * rows)].astype(jnp.float32))
            keep = (keys == queries) & (key_at + first <= query_at)
            bias_ref[slot * rows : (slot + 1) * rows, :] = jnp.where(keep, 0.0, NEG)
    flagged = flags_ref[...].astype(jnp.float32)
    count = jnp.sum(flagged, axis=1, keepdims=True)
    count_ref[...] = jnp.broadcast_to(count, count_ref.shape)
    keep = upright(flagged).astype(jnp.bfloat16)
    copies[3].wait()
    for h in range(up_ref.shape[1] // HEAD_DIM):
        cols = slice(h * HEAD_DIM, (h + 1) * HEAD_DIM)
        cots_ref[:, cols] = up_ref[:, cols] * keep
    for copy in copies[4:]:
        copy.wait()


def add_kernel(left_ref, right_ref, out_ref):
    out_ref[...] = left_ref[...] + right_ref[...]


def gain_kernel(tokens, left_ref, right_ref, out_ref):
    out_ref[...] = tokens / jnp.maximum(left_ref[...] + right_ref[...], 1.0)


def near_kernel(plan, bias_ref, q_ref, mid_ref, y_ref, own_ref, grad_ref, *refs):
    group, heads, factor, _ = plan
    acc_ref, peak_ref, sum_ref, grad_out, scores_buf, expo_buf, sem = refs
    copy = pltpu.make_async_copy(grad_ref, grad_out, sem)
    copy.start()
    rows = q_ref.shape[0]
    window = (mid_ref, y_ref, own_ref)

    def block(columns):
        return jnp.concatenate([ref[:, columns] for ref in window], axis=0)

    def scores(g):
        keys = block(column(g * HEAD_DIM))
        scores_buf[g % 2] = contract(keys, stacked_heads(q_ref, g, group), 1, 1)

    def softmax(g):
        for t in range(group):
            cols = slice(t * rows, (t + 1) * rows)
            marked = scores_buf[g % 2, :, cols] * factor + bias_ref[2 * rows :, :]
            peak = jnp.max(marked, axis=0, keepdims=True)
            expo = jnp.exp2(marked - peak)
            expo_buf[g % 2, :, cols] = expo.astype(expo_buf.dtype)
            peak_ref[g, :, cols] = peak
            sum_ref[g, :, cols] = jnp.sum(expo, axis=0, keepdims=True)

    def output(g):
        acc_ref[g] = contract(block(column((heads + g) * HEAD_DIM)), expo_buf[g % 2], 0, 0)

    staged(heads, scores, softmax, output)
    copy.wait()


def far_forward_kernel(plan, odd_ref, bias_ref, q_ref, far_ref, far_x_ref, near_x_ref, *refs):
    group, heads, factor, _ = plan
    acc_ref, peak_ref, sum_ref, out_ref, scores_buf, expo_buf = refs
    odd = odd_ref[0]
    rows = q_ref.shape[0]
    parts = {}

    def block(columns):
        x_slot = jnp.where(odd == 1, near_x_ref[:, columns], far_x_ref[:, columns])
        return jnp.concatenate([far_ref[:, columns], x_slot], axis=0)

    def scores(g):
        keys = block(column(g * HEAD_DIM))
        scores_buf[g % 2] = contract(keys, stacked_heads(q_ref, g, group), 1, 1)

    def softmax(g):
        parts[g] = []
        for t in range(group):
            cols = slice(t * rows, (t + 1) * rows)
            marked = scores_buf[g % 2, :, cols] * factor + bias_ref[: 2 * rows, :]
            near = peak_ref[g, :, cols]
            peak = jnp.maximum(near, jnp.max(marked, axis=0, keepdims=True))
            expo = jnp.exp2(marked - peak)
            expo_buf[g % 2, :, cols] = expo.astype(expo_buf.dtype)
            kept = jnp.exp2(near - peak)
            total = sum_ref[g, :, cols] * kept + jnp.sum(expo, axis=0, keepdims=True)
            parts[g].append((kept / total, 1.0 / total))

    def output(g):
        out = contract(block(column((heads + g) * HEAD_DIM)), expo_buf[g % 2], 0, 0)
        for t, (kept, inverse) in enumerate(parts[g]):
            cols = slice(t * rows, (t + 1) * rows)
            piece = acc_ref[g, :, cols] * kept + out[:, cols] * inverse
            out_ref[:, column((g * group + t) * HEAD_DIM)] = piece.T.astype(out_ref.dtype)

    staged(heads, scores, softmax, output)


def own_kernel(odd_ref, gain_ref, own_ref, other_ref, back_ref, *refs):
    *pair, out_ref, held, sems = refs
    copies = [pltpu.make_async_copy(*pair, sems.at[1])] if pair else []
    for copy in copies:
        copy.start()
    share = jnp.where(odd_ref[0] == 0, other_ref[...].astype(jnp.float32), 0.0)
    total = own_ref[...] + share + back_ref[...].astype(jnp.float32)
    gain = jnp.concatenate([gain_ref[...]] * (total.shape[1] // HEAD_DIM), axis=1)
    held[...] = (total * gain).astype(held.dtype)
    copies.append(pltpu.make_async_copy(held, out_ref, sems.at[0]))
    copies[-1].start()
    for copy in copies:
        copy.wait()


def probs_kernel(plan, odd_ref, bias_ref, q_ref, d_ref, *refs):
    group, heads, factor, _ = plan
    window, (p_ref, outs, scores_buf) = refs[:6], (refs[6], refs[7:-1], refs[-1])
    odd = odd_ref[0]
    rows = q_ref.shape[0]

    def scores(g):
        keys = gather_window(odd, window, column(g * HEAD_DIM))
        scores_buf[g % 2] = contract(keys, stacked_heads(q_ref, g, group), 1, 1)

    def softmax(g):
        soften(scores_buf.at[g % 2], bias_ref, p_ref.at[g], group, factor)

    def gradients(g):
        dv = contract(p_ref[g], stacked_heads(d_ref, g, group), 1, 0)
        for s, ref in enumerate(outs):
            ref[:, column(g * HEAD_DIM)] = dv[s * rows : (s + 1) * rows].astype(ref.dtype)

    staged(heads, scores, softmax, gradients)


def scores_kernel(plan, odd_ref, q_ref, d_ref, p_ref, *refs):
    group, heads, _, scale = plan
    window, (s_ref, far_ref, x_ref, probs_buf) = refs[:6], refs[6:]
    odd = odd_ref[0]
    rows = q_ref.shape[0]

    def products(g):
        values = gather_window(odd, window, column(g * HEAD_DIM))
        probs_buf[g % 2] = contract(values, stacked_heads(d_ref, g, group), 1, 1)

    def scores(g):
        for t in range(group):
            cols = slice(t * rows, (t + 1) * rows)
            d_probs = probs_buf[g % 2, :, cols]
            probs = p_ref[g, :, cols].astype(jnp.float32)
            delta = jnp.sum(probs * d_probs, axis=0, keepdims=True)
            s_ref[g, :, cols] = (probs * (d_probs - delta)).astype(s_ref.dtype)

    def gradients(g):
        cols = column(g * HEAD_DIM)
        dk = contract(s_ref[g, : 2 * rows, :], stacked_heads(q_ref, g, group), 1, 0) * scale
        far_ref[:, cols] = dk[:rows].astype(far_ref.dtype)
        x_ref[:, cols] = dk[rows:].astype(x_ref.dtype)

    staged(heads, products, scores, gradients)


def keys_kernel(plan, q_ref, s_ref, mid_ref, y_ref, own_ref):
    group, heads, _, scale = plan
    rows = q_ref.shape[0]

    def one(g, carry):
        cols = column(g * HEAD_DIM)
        queries = stacked_heads(q_ref, g, group)
        dk = contract(s_ref[g, 2 * rows :, :], queries, 1, 0) * scale
        for s, ref in enumerate((mid_ref, y_ref, own_ref)):
            ref[:, cols] = dk[s * rows : (s + 1) * rows].astype(ref.dtype)
        return carry

    lax.fori_loop(0, heads, one, 0, unroll=4)


def queries_kernel(plan, odd_ref, gain_ref, s_ref, *refs):
    group, heads, _, scale = plan
    window, dq_ref = refs[:6], refs[6]
    odd = odd_ref[0]
    rows = gain_ref.shape[1]
    gain = gain_ref[...] * scale

    def one(g, carry):
        keys = gather_window(odd, window, column(g * HEAD_DIM))
        dq = contract(keys, s_ref[g], 0, 0)
        for t in range(group):
            piece = dq[:, t * rows : (t + 1) * rows].T * gain
            dq_ref[:, column((g * group + t) * HEAD_DIM)] = piece.astype(dq_ref.dtype)
        return carry

    lax.fori_loop(0, heads, one, 0, unroll=4)


def far_kernel(odd_ref, far_ref, x_ref, out_ref):
    share = jnp.where(odd_ref[0] == 1, x_ref[...].astype(jnp.float32), 0.0)
    out_ref[...] = (far_ref[...] + share).astype(out_ref.dtype)


def mid_kernel(mid_ref, y_ref, back_ref, out_ref):
    total = mid_ref[...] + y_ref[...].astype(jnp.float32) + back_ref[...].astype(jnp.float32)
    out_ref[...] = total.astype(out_ref.dtype)


def call(kernel, outs, smem, args, in_hbm=(), out_hbm=(), scratch=()):
    vmem = pl.BlockSpec(memory_space=pltpu.VMEM)
    scalar = pl.BlockSpec(memory_space=pltpu.SMEM)
    hbm = pl.BlockSpec(memory_space=pltpu.HBM)
    args = [
        pltpu.with_memory_space_constraint(x, pltpu.HBM) if i in in_hbm else x
        for i, x in enumerate(args)
    ]
    return pl.pallas_call(
        kernel,
        out_shape=tuple(outs) if len(outs) > 1 else outs[0],
        in_specs=[scalar] * len(smem)
        + [hbm if i in in_hbm else vmem for i in range(len(args))],
        out_specs=tuple(hbm if i in out_hbm else vmem for i in range(len(outs)))
        if len(outs) > 1
        else (hbm if out_hbm else vmem),
        scratch_shapes=list(scratch),
        compiler_params=pltpu.CompilerParams(vmem_limit_bytes=VMEM_LIMIT),
    )(*smem, *args)


def fetch_window(block, mid):
    near_x = swapped(block)
    far = shifted(mid, 2, second=True)
    near_y = swapped(mid)
    far_x = swapped(far)
    return far, far_x, mid, near_y, block, near_x


def body(q_next, k_next, v_next, seg_next, q_prev, k_prev, v_prev, seg_prev, upstream, flags):
    rows = q_next.shape[0]
    heads_all = q_next.shape[1] // HEAD_DIM
    heads = k_next.shape[1] // HEAD_DIM
    group = heads_all // heads
    seq_size, fsdp_size = lax.axis_size("seq"), lax.axis_size("fsdp")
    tokens = rows * fsdp_size * seq_size
    assert seq_size % 2 == 0 and SEG_MOST <= 4 * rows and rows == HEAD_DIM
    scale = HEAD_DIM ** (-0.5)
    plan = (group, heads, scale * math.log2(math.e), scale)
    index = lax.axis_index("seq").astype(jnp.int32).reshape(1)
    odd = index % 2
    b16, f32 = jnp.bfloat16, jnp.float32

    def sds(shape, dtype):
        return jax.ShapeDtypeStruct(shape, dtype)

    k_shape, v_shape = k_prev.shape, v_prev.shape
    wide = group * rows
    scores_scratch = pltpu.VMEM((2, SLOTS * rows, wide), f32)

    keys_out, values_out = (shifted(x, 2) for x in (k_prev, v_prev))
    bias_shape = sds((SLOTS * rows, rows), f32)
    line = sds((1, HEAD_DIM), f32)
    staged = (seg_prev, seg_next, flags, upstream, q_prev, k_prev, v_prev, q_next, k_next, v_next)
    bias_prev, bias_next, count, cots, q_prev, k_here, v_here, q_next, kv_next = call(
        prep_kernel,
        (
            bias_shape,
            bias_shape,
            line,
            sds(upstream.shape, b16),
            sds(q_prev.shape, b16),
            sds(k_shape, b16),
            sds(v_shape, b16),
            sds(q_next.shape, b16),
            sds((rows, 2 * k_next.shape[1]), b16),
        ),
        (index,),
        staged,
        in_hbm=range(len(staged)),
        scratch=tuple(pltpu.VMEM(x.shape, x.dtype) for x in staged[:4])
        + (pltpu.SemaphoreType.DMA((len(staged),)),),
    )
    keys = fetch_window(k_here, keys_out)
    values = fetch_window(v_here, values_out)
    window_next = fetch_window(kv_next, shifted(kv_next, 2))
    steps = [("fsdp", 1 << i) for i in range((fsdp_size - 1).bit_length())]
    steps += [("seq", 1 << i) for i in range(1, (seq_size - 1).bit_length())] + [("seq", 1)]
    for at, (axis, step) in enumerate(steps):
        route = [(i, i ^ step) for i in range(lax.axis_size(axis))]
        other = lax.ppermute(count, axis, route)
        last = at == len(steps) - 1
        kernel = functools.partial(gain_kernel, tokens) if last else add_kernel
        count = call(kernel, (line,), (), (count, other))
    gain = count

    probs, far_v, x_v, mid_v, y_v, own_v = call(
        functools.partial(probs_kernel, plan),
        (
            sds((heads, SLOTS * rows, wide), b16),
            sds(v_shape, f32),
            sds(v_shape, b16),
            sds(v_shape, f32),
            sds(v_shape, b16),
            sds(v_shape, f32),
        ),
        (odd,),
        (bias_prev, q_prev, cots, *keys),
        scratch=(scores_scratch,),
    )
    x_v, y_v = swapped(x_v), swapped(y_v)
    far_v = call(far_kernel, (sds(v_shape, b16),), (odd,), (far_v, x_v))
    far_v = returned(far_v)

    d_scores, far_k, x_k = call(
        functools.partial(scores_kernel, plan),
        (sds(probs.shape, b16), sds(k_shape, f32), sds(k_shape, b16)),
        (odd,),
        (q_prev, cots, probs, *values),
        scratch=(scores_scratch,),
    )
    x_k = swapped(x_k)
    far_k = call(far_kernel, (sds(k_shape, b16),), (odd,), (far_k, x_k))
    far_k = returned(far_k)

    mid_v = call(mid_kernel, (sds(v_shape, b16),), (), (mid_v, y_v, far_v))
    mid_v = shifted(mid_v, -2)
    mid_k, y_k, own_k = call(
        functools.partial(keys_kernel, plan),
        (sds(k_shape, f32), sds(k_shape, b16), sds(k_shape, f32)),
        (),
        (q_prev, d_scores),
    )
    y_k = swapped(y_k)
    grad_q = call(
        functools.partial(queries_kernel, plan),
        (sds(q_prev.shape, b16),),
        (odd,),
        (gain, d_scores, *keys),
    )
    mid_k = call(mid_kernel, (sds(k_shape, b16),), (), (mid_k, y_k, far_k))
    mid_k = shifted(mid_k, -2)

    far_next, far_x_next, mid_next, y_next, own_next, near_x_next = window_next

    def buffers(blocks):
        return tuple(pltpu.VMEM((2, blocks * rows, wide), dtype) for dtype in (f32, b16))

    *near, grad_q = call(
        functools.partial(near_kernel, plan),
        (
            sds((heads, HEAD_DIM, wide), f32),
            sds((heads, 1, wide), f32),
            sds((heads, 1, wide), f32),
            sds(q_prev.shape, b16),
        ),
        (),
        (bias_next, q_next, mid_next, y_next, own_next, grad_q),
        out_hbm=(3,),
        scratch=buffers(3) + (pltpu.SemaphoreType.DMA,),
    )
    attn_next = call(
        functools.partial(far_forward_kernel, plan),
        (sds(q_next.shape, b16),),
        (odd,),
        (bias_next, q_next, far_next, far_x_next, near_x_next, *near),
        scratch=buffers(2),
    )
    held = (pltpu.VMEM(k_shape, b16), pltpu.SemaphoreType.DMA((2,)))
    grad_v = call(
        own_kernel,
        (sds(v_shape, b16),),
        (odd,),
        (gain, own_v, x_v, mid_v),
        out_hbm=(0,),
        scratch=held,
    )
    attn_next, grad_k = call(
        own_kernel,
        (sds(q_next.shape, b16), sds(k_shape, b16)),
        (odd,),
        (gain, own_k, x_k, mid_k, attn_next),
        out_hbm=(0, 1),
        scratch=held,
    )
    return (attn_next, grad_q, grad_k, grad_v)


def solution(mesh):
    tokens = P(("fsdp", "seq"), None)
    ids = P("fsdp", None)
    return jax.shard_map(
        body,
        mesh=mesh,
        in_specs=(tokens, tokens, tokens, ids) * 2 + (tokens, P("fsdp", "seq")),
        out_specs=(tokens,) * 4,
        check_vma=False,
    )
```

```python
import functools
import math

import jax
import jax.numpy as jnp
from jax import lax
from jax.experimental import pallas as pl
from jax.experimental.pallas import tpu as pltpu
from jax.sharding import PartitionSpec as P


HEAD_DIM = 128
SEG_MOST = 512
SLOTS = 5
NEG = -1e30
VMEM_LIMIT = 12 << 20


def shifted(block, step, second=False):
    size = lax.axis_size("seq")
    route = [(i, i + step) for i in range(size) if 0 <= i + step < size]
    if second:
        route = [(i, j) for i, j in route if 0 <= i - abs(step)]
    return lax.ppermute(block, "seq", route)


def returned(block):
    route = [(i, i - 2) for i in range(4, lax.axis_size("seq"))]
    return lax.ppermute(block, "seq", route)


def swapped(block):
    route = [(i, i ^ 1) for i in range(lax.axis_size("seq"))]
    return lax.ppermute(block, "seq", route)


def column(start):
    return pl.ds(pl.multiple_of(start, HEAD_DIM), HEAD_DIM)


def gather_window(odd, refs, columns):
    far, far_x, mid, near_y, own, near_x = refs
    x_slot = jnp.where(odd == 1, near_x[:, columns], far_x[:, columns])
    return jnp.concatenate(
        [far[:, columns], x_slot, mid[:, columns], near_y[:, columns], own[:, columns]], axis=0
    )


def stacked_heads(ref, kv_head, group):
    return jnp.concatenate(
        [ref[:, column((kv_head * group + t) * HEAD_DIM)] for t in range(group)], axis=0
    )


def contract(left, right, left_dim, right_dim):
    return lax.dot_general(
        left,
        right,
        (((left_dim,), (right_dim,)), ((), ())),
        preferred_element_type=jnp.float32,
    )


def staged(count, *stages):
    for step in range(count + len(stages) - 1):
        for depth in reversed(range(len(stages))):
            if 0 <= step - depth < count:
                stages[depth](step - depth)


def masked_scores(keys, queries, bias_ref, group, factor, out_ref):
    scores = contract(keys, queries, 1, 1) * factor
    scores = scores + jnp.concatenate([bias_ref[...]] * group, axis=1)
    out_ref[...] = scores
    return jnp.max(scores, axis=0, keepdims=True)


def soften(scores_ref, peaks, expo_ref, group):
    rows = peaks.shape[1] // group
    inverses = []
    for t in range(group):
        cols = slice(t * rows, (t + 1) * rows)
        expo = jnp.exp2(scores_ref[:, cols] - peaks[:, cols])
        expo_ref[:, cols] = expo.astype(expo_ref.dtype)
        inverses.append(1.0 / jnp.sum(expo, axis=0, keepdims=True))
    return inverses


def upright(row):
    return jnp.broadcast_to(row, (HEAD_DIM, HEAD_DIM)).T


def prep_kernel(index_ref, *refs):
    prev_hbm, next_hbm, flags_hbm, up_hbm, qp_hbm, kp_hbm, vp_hbm, qn_hbm, kn_hbm, vn_hbm = refs[:10]
    bias_prev_ref, bias_next_ref, count_ref, cots_ref, qp_ref, kp_ref, vp_ref = refs[10:17]
    qn_ref, kv_ref, prev_ref, next_ref, flags_ref, up_ref, sems = refs[17:]
    width = kn_hbm.shape[1]
    moves = (
        (prev_hbm, prev_ref),
        (next_hbm, next_ref),
        (flags_hbm, flags_ref),
        (up_hbm, up_ref),
        (qp_hbm, qp_ref),
        (kp_hbm, kp_ref),
        (vp_hbm, vp_ref),
        (kn_hbm, kv_ref.at[:, :width]),
        (vn_hbm, kv_ref.at[:, width:]),
        (qn_hbm, qn_ref),
    )
    copies = [pltpu.make_async_copy(a, b, sems.at[i]) for i, (a, b) in enumerate(moves)]
    for copy in copies:
        copy.start()
    index = index_ref[0]
    odd = index % 2
    rows = flags_ref.shape[1]
    far = jnp.iinfo(jnp.int32).max // 2
    key_at = lax.broadcasted_iota(jnp.int32, (rows, rows), 0)
    query_at = lax.broadcasted_iota(jnp.int32, (rows, rows), 1)
    for copy in copies[:3]:
        copy.wait()
    for seg_ref, bias_ref in ((prev_ref, bias_prev_ref), (next_ref, bias_next_ref)):
        queries = seg_ref[:, column(index * rows)].astype(jnp.float32)
        for slot, back in enumerate((4, 3 - 2 * odd, 2, 1 + 2 * odd, 0)):
            block = index - back
            first = jnp.where(block >= 0, -back * rows, far)
            keys = upright(seg_ref[:, column(jnp.maximum(block, 0) * rows)].astype(jnp.float32))
            keep = (keys == queries) & (key_at + first <= query_at)
            bias_ref[slot * rows : (slot + 1) * rows, :] = jnp.where(keep, 0.0, NEG)
    flagged = flags_ref[...].astype(jnp.float32)
    count = jnp.sum(flagged, axis=1, keepdims=True)
    count_ref[...] = jnp.broadcast_to(count, count_ref.shape)
    keep = upright(flagged).astype(jnp.bfloat16)
    copies[3].wait()
    for h in range(up_ref.shape[1] // HEAD_DIM):
        cols = slice(h * HEAD_DIM, (h + 1) * HEAD_DIM)
        cots_ref[:, cols] = up_ref[:, cols] * keep
    for copy in copies[4:]:
        copy.wait()


def add_kernel(left_ref, right_ref, out_ref):
    out_ref[...] = left_ref[...] + right_ref[...]


def gain_kernel(tokens, left_ref, right_ref, out_ref):
    out_ref[...] = tokens / jnp.maximum(left_ref[...] + right_ref[...], 1.0)


def near_kernel(plan, bias_ref, q_ref, mid_ref, y_ref, own_ref, grad_ref, *refs):
    group, heads, factor, _ = plan
    acc_ref, peak_ref, sum_ref, grad_out, scores_buf, expo_buf, sem = refs
    copy = pltpu.make_async_copy(grad_ref, grad_out, sem)
    copy.start()
    rows = q_ref.shape[0]
    window = (mid_ref, y_ref, own_ref)

    def block(columns):
        return jnp.concatenate([ref[:, columns] for ref in window], axis=0)

    def scores(g):
        keys = block(column(g * HEAD_DIM))
        scores_buf[g % 2] = contract(keys, stacked_heads(q_ref, g, group), 1, 1)

    def softmax(g):
        for t in range(group):
            cols = slice(t * rows, (t + 1) * rows)
            marked = scores_buf[g % 2, :, cols] * factor + bias_ref[2 * rows :, :]
            peak = jnp.max(marked, axis=0, keepdims=True)
            expo = jnp.exp2(marked - peak)
            expo_buf[g % 2, :, cols] = expo.astype(expo_buf.dtype)
            peak_ref[g, :, cols] = peak
            sum_ref[g, :, cols] = jnp.sum(expo, axis=0, keepdims=True)

    def output(g):
        acc_ref[g] = contract(block(column((heads + g) * HEAD_DIM)), expo_buf[g % 2], 0, 0)

    staged(heads, scores, softmax, output)
    copy.wait()


def far_forward_kernel(plan, odd_ref, bias_ref, q_ref, far_ref, far_x_ref, near_x_ref, *refs):
    group, heads, factor, _ = plan
    acc_ref, peak_ref, sum_ref, out_ref, scores_buf, expo_buf = refs
    odd = odd_ref[0]
    rows = q_ref.shape[0]
    parts = {}

    def block(columns):
        x_slot = jnp.where(odd == 1, near_x_ref[:, columns], far_x_ref[:, columns])
        return jnp.concatenate([far_ref[:, columns], x_slot], axis=0)

    def scores(g):
        keys = block(column(g * HEAD_DIM))
        scores_buf[g % 2] = contract(keys, stacked_heads(q_ref, g, group), 1, 1)

    def softmax(g):
        parts[g] = []
        for t in range(group):
            cols = slice(t * rows, (t + 1) * rows)
            marked = scores_buf[g % 2, :, cols] * factor + bias_ref[: 2 * rows, :]
            near = peak_ref[g, :, cols]
            peak = jnp.maximum(near, jnp.max(marked, axis=0, keepdims=True))
            expo = jnp.exp2(marked - peak)
            expo_buf[g % 2, :, cols] = expo.astype(expo_buf.dtype)
            kept = jnp.exp2(near - peak)
            total = sum_ref[g, :, cols] * kept + jnp.sum(expo, axis=0, keepdims=True)
            parts[g].append((kept / total, 1.0 / total))

    def output(g):
        out = contract(block(column((heads + g) * HEAD_DIM)), expo_buf[g % 2], 0, 0)
        for t, (kept, inverse) in enumerate(parts[g]):
            cols = slice(t * rows, (t + 1) * rows)
            piece = acc_ref[g, :, cols] * kept + out[:, cols] * inverse
            out_ref[:, column((g * group + t) * HEAD_DIM)] = piece.T.astype(out_ref.dtype)

    staged(heads, scores, softmax, output)


def own_kernel(odd_ref, gain_ref, own_ref, other_ref, back_ref, *refs):
    *pair, out_ref, held, sems = refs
    copies = [pltpu.make_async_copy(*pair, sems.at[1])] if pair else []
    for copy in copies:
        copy.start()
    share = jnp.where(odd_ref[0] == 0, other_ref[...].astype(jnp.float32), 0.0)
    total = own_ref[...] + share + back_ref[...].astype(jnp.float32)
    gain = jnp.concatenate([gain_ref[...]] * (total.shape[1] // HEAD_DIM), axis=1)
    held[...] = (total * gain).astype(held.dtype)
    copies.append(pltpu.make_async_copy(held, out_ref, sems.at[0]))
    copies[-1].start()
    for copy in copies:
        copy.wait()


def probs_kernel(plan, odd_ref, bias_ref, q_ref, d_ref, *refs):
    group, heads, factor, _ = plan
    window, (p_ref, c_ref, i_ref), outs, scores_buf = refs[:6], refs[6:9], refs[9:-1], refs[-1]
    odd = odd_ref[0]
    rows = q_ref.shape[0]
    peaks = {}

    def scores(g):
        keys = gather_window(odd, window, column(g * HEAD_DIM))
        queries = stacked_heads(q_ref, g, group)
        buf = scores_buf.at[g % 2]
        peaks[g] = masked_scores(keys, queries, bias_ref, group, factor, buf)

    def softmax(g):
        inverses = soften(scores_buf.at[g % 2], peaks[g], p_ref.at[g], group)
        for t, inverse in enumerate(inverses):
            cots = d_ref[:, column((g * group + t) * HEAD_DIM)].astype(jnp.float32)
            c_ref[g, t * rows : (t + 1) * rows, :] = (cots * upright(inverse)).astype(c_ref.dtype)
            i_ref[g, :, t * rows : (t + 1) * rows] = inverse

    def gradients(g):
        dv = contract(p_ref[g], c_ref[g], 1, 0)
        for s, ref in enumerate(outs):
            ref[:, column(g * HEAD_DIM)] = dv[s * rows : (s + 1) * rows].astype(ref.dtype)

    staged(heads, scores, softmax, gradients)


def scores_kernel(plan, odd_ref, q_ref, p_ref, c_ref, i_ref, *refs):
    group, heads, _, scale = plan
    window, (s_ref, far_ref, x_ref, probs_buf) = refs[:6], refs[6:]
    odd = odd_ref[0]
    rows = q_ref.shape[0]

    def products(g):
        values = gather_window(odd, window, column(g * HEAD_DIM))
        probs_buf[g % 2] = contract(values, c_ref[g], 1, 1)

    def scores(g):
        for t in range(group):
            cols = slice(t * rows, (t + 1) * rows)
            d_probs = probs_buf[g % 2, :, cols]
            probs = p_ref[g, :, cols].astype(jnp.float32)
            delta = jnp.sum(probs * d_probs, axis=0, keepdims=True) * i_ref[g, :, cols]
            s_ref[g, :, cols] = (probs * (d_probs - delta)).astype(s_ref.dtype)

    def gradients(g):
        cols = column(g * HEAD_DIM)
        dk = contract(s_ref[g, : 2 * rows, :], stacked_heads(q_ref, g, group), 1, 0) * scale
        far_ref[:, cols] = dk[:rows].astype(far_ref.dtype)
        x_ref[:, cols] = dk[rows:].astype(x_ref.dtype)

    staged(heads, products, scores, gradients)


def keys_kernel(plan, q_ref, s_ref, mid_ref, y_ref, own_ref):
    group, heads, _, scale = plan
    rows = q_ref.shape[0]

    def one(g, carry):
        cols = column(g * HEAD_DIM)
        queries = stacked_heads(q_ref, g, group)
        dk = contract(s_ref[g, 2 * rows :, :], queries, 1, 0) * scale
        for s, ref in enumerate((mid_ref, y_ref, own_ref)):
            ref[:, cols] = dk[s * rows : (s + 1) * rows].astype(ref.dtype)
        return carry

    lax.fori_loop(0, heads, one, 0, unroll=4)


def queries_kernel(plan, odd_ref, gain_ref, s_ref, *refs):
    group, heads, _, scale = plan
    window, dq_ref = refs[:6], refs[6]
    odd = odd_ref[0]
    rows = gain_ref.shape[1]
    gain = gain_ref[...] * scale

    def one(g, carry):
        keys = gather_window(odd, window, column(g * HEAD_DIM))
        dq = contract(keys, s_ref[g], 0, 0)
        for t in range(group):
            piece = dq[:, t * rows : (t + 1) * rows].T * gain
            dq_ref[:, column((g * group + t) * HEAD_DIM)] = piece.astype(dq_ref.dtype)
        return carry

    lax.fori_loop(0, heads, one, 0, unroll=4)


def far_kernel(odd_ref, far_ref, x_ref, out_ref):
    share = jnp.where(odd_ref[0] == 1, x_ref[...].astype(jnp.float32), 0.0)
    out_ref[...] = (far_ref[...] + share).astype(out_ref.dtype)


def mid_kernel(mid_ref, y_ref, back_ref, out_ref):
    total = mid_ref[...] + y_ref[...].astype(jnp.float32) + back_ref[...].astype(jnp.float32)
    out_ref[...] = total.astype(out_ref.dtype)


def call(kernel, outs, smem, args, in_hbm=(), out_hbm=(), scratch=()):
    vmem = pl.BlockSpec(memory_space=pltpu.VMEM)
    scalar = pl.BlockSpec(memory_space=pltpu.SMEM)
    hbm = pl.BlockSpec(memory_space=pltpu.HBM)
    args = [
        pltpu.with_memory_space_constraint(x, pltpu.HBM) if i in in_hbm else x
        for i, x in enumerate(args)
    ]
    return pl.pallas_call(
        kernel,
        out_shape=tuple(outs) if len(outs) > 1 else outs[0],
        in_specs=[scalar] * len(smem)
        + [hbm if i in in_hbm else vmem for i in range(len(args))],
        out_specs=tuple(hbm if i in out_hbm else vmem for i in range(len(outs)))
        if len(outs) > 1
        else (hbm if out_hbm else vmem),
        scratch_shapes=list(scratch),
        compiler_params=pltpu.CompilerParams(vmem_limit_bytes=VMEM_LIMIT),
    )(*smem, *args)


def fetch_window(block, mid):
    near_x = swapped(block)
    far = shifted(mid, 2, second=True)
    near_y = swapped(mid)
    far_x = swapped(far)
    return far, far_x, mid, near_y, block, near_x


def body(q_next, k_next, v_next, seg_next, q_prev, k_prev, v_prev, seg_prev, upstream, flags):
    rows = q_next.shape[0]
    heads_all = q_next.shape[1] // HEAD_DIM
    heads = k_next.shape[1] // HEAD_DIM
    group = heads_all // heads
    seq_size, fsdp_size = lax.axis_size("seq"), lax.axis_size("fsdp")
    tokens = rows * fsdp_size * seq_size
    assert seq_size % 2 == 0 and SEG_MOST <= 4 * rows and rows == HEAD_DIM
    scale = HEAD_DIM ** (-0.5)
    plan = (group, heads, scale * math.log2(math.e), scale)
    index = lax.axis_index("seq").astype(jnp.int32).reshape(1)
    odd = index % 2
    b16, f32 = jnp.bfloat16, jnp.float32

    def sds(shape, dtype):
        return jax.ShapeDtypeStruct(shape, dtype)

    k_shape, v_shape = k_prev.shape, v_prev.shape
    wide = group * rows
    scores_scratch = pltpu.VMEM((2, SLOTS * rows, wide), f32)

    keys_out, values_out = (shifted(x, 2) for x in (k_prev, v_prev))
    bias_shape = sds((SLOTS * rows, rows), f32)
    line = sds((1, HEAD_DIM), f32)
    staged = (seg_prev, seg_next, flags, upstream, q_prev, k_prev, v_prev, q_next, k_next, v_next)
    bias_prev, bias_next, count, cots, q_prev, k_here, v_here, q_next, kv_next = call(
        prep_kernel,
        (
            bias_shape,
            bias_shape,
            line,
            sds(upstream.shape, b16),
            sds(q_prev.shape, b16),
            sds(k_shape, b16),
            sds(v_shape, b16),
            sds(q_next.shape, b16),
            sds((rows, 2 * k_next.shape[1]), b16),
        ),
        (index,),
        staged,
        in_hbm=range(len(staged)),
        scratch=tuple(pltpu.VMEM(x.shape, x.dtype) for x in staged[:4])
        + (pltpu.SemaphoreType.DMA((len(staged),)),),
    )
    keys = fetch_window(k_here, keys_out)
    values = fetch_window(v_here, values_out)
    window_next = fetch_window(kv_next, shifted(kv_next, 2))
    steps = [("fsdp", 1 << i) for i in range((fsdp_size - 1).bit_length())]
    steps += [("seq", 1 << i) for i in range(1, (seq_size - 1).bit_length())] + [("seq", 1)]
    for at, (axis, step) in enumerate(steps):
        route = [(i, i ^ step) for i in range(lax.axis_size(axis))]
        other = lax.ppermute(count, axis, route)
        last = at == len(steps) - 1
        kernel = functools.partial(gain_kernel, tokens) if last else add_kernel
        count = call(kernel, (line,), (), (count, other))
    gain = count

    probs, shares, inverses, far_v, x_v, mid_v, y_v, own_v = call(
        functools.partial(probs_kernel, plan),
        (
            sds((heads, SLOTS * rows, wide), b16),
            sds((heads, wide, HEAD_DIM), b16),
            sds((heads, 1, wide), f32),
            sds(v_shape, f32),
            sds(v_shape, b16),
            sds(v_shape, f32),
            sds(v_shape, b16),
            sds(v_shape, f32),
        ),
        (odd,),
        (bias_prev, q_prev, cots, *keys),
        scratch=(scores_scratch,),
    )
    x_v, y_v = swapped(x_v), swapped(y_v)
    far_v = call(far_kernel, (sds(v_shape, b16),), (odd,), (far_v, x_v))
    far_v = returned(far_v)

    d_scores, far_k, x_k = call(
        functools.partial(scores_kernel, plan),
        (sds(probs.shape, b16), sds(k_shape, f32), sds(k_shape, b16)),
        (odd,),
        (q_prev, probs, shares, inverses, *values),
        scratch=(scores_scratch,),
    )
    x_k = swapped(x_k)
    far_k = call(far_kernel, (sds(k_shape, b16),), (odd,), (far_k, x_k))
    far_k = returned(far_k)

    mid_v = call(mid_kernel, (sds(v_shape, b16),), (), (mid_v, y_v, far_v))
    mid_v = shifted(mid_v, -2)
    mid_k, y_k, own_k = call(
        functools.partial(keys_kernel, plan),
        (sds(k_shape, f32), sds(k_shape, b16), sds(k_shape, f32)),
        (),
        (q_prev, d_scores),
    )
    y_k = swapped(y_k)
    grad_q = call(
        functools.partial(queries_kernel, plan),
        (sds(q_prev.shape, b16),),
        (odd,),
        (gain, d_scores, *keys),
    )
    mid_k = call(mid_kernel, (sds(k_shape, b16),), (), (mid_k, y_k, far_k))
    mid_k = shifted(mid_k, -2)

    far_next, far_x_next, mid_next, y_next, own_next, near_x_next = window_next

    def buffers(blocks):
        return tuple(pltpu.VMEM((2, blocks * rows, wide), dtype) for dtype in (f32, b16))

    *near, grad_q = call(
        functools.partial(near_kernel, plan),
        (
            sds((heads, HEAD_DIM, wide), f32),
            sds((heads, 1, wide), f32),
            sds((heads, 1, wide), f32),
            sds(q_prev.shape, b16),
        ),
        (),
        (bias_next, q_next, mid_next, y_next, own_next, grad_q),
        out_hbm=(3,),
        scratch=buffers(3) + (pltpu.SemaphoreType.DMA,),
    )
    attn_next = call(
        functools.partial(far_forward_kernel, plan),
        (sds(q_next.shape, b16),),
        (odd,),
        (bias_next, q_next, far_next, far_x_next, near_x_next, *near),
        scratch=buffers(2),
    )
    held = (pltpu.VMEM(k_shape, b16), pltpu.SemaphoreType.DMA((2,)))
    grad_v = call(
        own_kernel,
        (sds(v_shape, b16),),
        (odd,),
        (gain, own_v, x_v, mid_v),
        out_hbm=(0,),
        scratch=held,
    )
    attn_next, grad_k = call(
        own_kernel,
        (sds(q_next.shape, b16), sds(k_shape, b16)),
        (odd,),
        (gain, own_k, x_k, mid_k, attn_next),
        out_hbm=(0, 1),
        scratch=held,
    )
    return (attn_next, grad_q, grad_k, grad_v)


def solution(mesh):
    tokens = P(("fsdp", "seq"), None)
    ids = P("fsdp", None)
    return jax.shard_map(
        body,
        mesh=mesh,
        in_specs=(tokens, tokens, tokens, ids) * 2 + (tokens, P("fsdp", "seq")),
        out_specs=(tokens,) * 4,
        check_vma=False,
    )
```
